256 devices in a mesh: row: 32 (over x, z_hi, y), col: 8 (over z_lo, core).
Axes of the slice: x: 4, y: 4, z: 8 (z_hi: 2, z_lo: 4; z = z_hi * 4 + z_lo), core: 2. Of those that a mesh axis runs over, the one named last changes fastest.
Arguments:
- lanczos_now: float32 [1, 256, 1024], P(None, 'row', 'col'), may hold values from -80 to 80, as said below
- lanczos_prev: float32 [1, 256, 1024], P(None, 'row', 'col'), may hold values from -6 to 6
- beta_prev: float32 [1], replicated, may hold values from 0.3 to 1.5
- valence_energy: float32 [256], P('row'), may hold values from -1.5 to -0.5
- conduction_energy: float32 [1024], P('col'), may hold values from 0.5 to 2.5
- valence_panel: float32 [16384, 256], P(('row', 'col')), may hold values from -0.375 to 0.375
- conduction_panel: float32 [16384, 1024], P(('row', 'col')), may hold values from -0.1875 to 0.1875
- screened_coulomb: float32 [16384, 16384], P('row', 'col'), may hold values from -0.046875 to 0.046875
- bare_coulomb: float32 [16384, 16384], P('row', 'col'), may hold values from -0.046875 to 0.046875
Outputs:
- lanczos_next: float32 [1, 256, 1024], P(None, 'row', 'col')
- coefficients: float32 [1, 2], replicated
The draws below stay inside these ranges and needn't reach their ends.
Inputs may be any that keep to these rules, and one draw needn't show every extreme that they name: `lanczos_now`: real entries; the vectors of a chain are not normalized.
All inputs are finite; a program needn't handle non-finite values.
Results may differ from the reference program's by a relative error of at most 0.0002.
Values sent between devices are 32-bit elements; how exact they have to be, the bound alone decides.
No kernel may reach another device: no remote copies, remote signals or barrier semaphores. Data moves between devices by JAX's collectives and lax.ppermute only.
A program may use at most 128 MiB of HBM per device.

```python
import math
import jax
import jax.numpy as jnp
from jax import lax

V = 256
C = 1024
NP = 16384
NVEC = 1


def draw_lanczos_now(key, part):
    noise_key, column_key = jax.random.split(key, 2)
    base = jnp.clip(jax.random.normal(noise_key, (NVEC, V, C), jnp.float32), -6.0, 6.0)
    position = jnp.arange(V, dtype=jnp.float32) / (V - 1)
    row_scale = 10.0 ** (position - 0.5)
    column_scale = jnp.exp(jax.random.uniform(column_key, (C,), jnp.float32, 0.0, math.log(3.0)))
    return base * row_scale[None, :, None] * column_scale[None, None, :]


def block_levels(key, dims, pieces, low, top_value):
    def one(axis_at, parts):
        steps = jax.random.uniform(jax.random.fold_in(jax.random.fold_in(key, 6), axis_at), (parts,), jnp.float32, low / len(pieces), top_value / len(pieces))
        return jnp.repeat(jnp.exp(steps), dims[axis_at] // parts).reshape((-1,) + (1,) * (len(dims) - axis_at - 1))

    factor_of = one(*pieces[0])
    for cut in pieces[1:]:
        factor_of = factor_of * one(*cut)
    return factor_of


def normal_values(stream_key, extent, width, limit, shards=(), kind=jnp.bfloat16):
    loudness = block_levels(stream_key, extent, shards, -0.22, 0.18) if shards else 1.0
    entries = jax.random.normal(stream_key, extent, jnp.float32) * width * loudness
    return jnp.minimum(jnp.maximum(entries, -limit), limit).astype(kind)


def setup_inputs(seed: int = 0) -> dict:
    key_of = jax.random.split(jax.random.key(seed), 10)
    return {
        "lanczos_now": draw_lanczos_now(jax.random.fold_in(key_of[9], 71), 0),
        "lanczos_prev": normal_values(key_of[1], (NVEC, V, C), 1.0, 6.0, ((1, 32), (2, 8)), jnp.float32),
        "beta_prev": jnp.clip(jnp.exp(jax.random.uniform(key_of[2], (NVEC,), jnp.float32, math.log(0.3), math.log(1.5))), 0.3, 1.5),
        "valence_energy": jnp.clip(-1.5 + 1.0 * jax.random.uniform(key_of[3], (V,), jnp.float32) ** block_levels(key_of[3], (V,), ((0, 32),), -0.2, 0.2), -1.5, -0.5),
        "conduction_energy": jnp.clip(0.5 + 2.0 * jax.random.uniform(key_of[4], (C,), jnp.float32) ** block_levels(key_of[4], (C,), ((0, 8),), -0.2, 0.2), 0.5, 2.5),
        "valence_panel": normal_values(key_of[5], (NP, V), V ** -0.5, 0.375, ((0, 256),), jnp.float32),
        "conduction_panel": normal_values(key_of[6], (NP, C), C ** -0.5, 0.1875, ((0, 256),), jnp.float32),
        "screened_coulomb": normal_values(key_of[7], (NP, NP), NP ** -0.5, 0.046875, ((0, 32), (1, 8)), jnp.float32),
        "bare_coulomb": normal_values(key_of[8], (NP, NP), NP ** -0.5, 0.046875, ((0, 32), (1, 8)), jnp.float32),
    }


precise = lax.Precision.HIGHEST
epsilon = 1e-06

def reference(lanczos_now, lanczos_prev, beta_prev, valence_energy, conduction_energy, valence_panel, conduction_panel, screened_coulomb, bare_coulomb):
    products = jnp.einsum('nv,kvc->knc', valence_panel, lanczos_now, precision=precise)
    density = lax.optimization_barrier(jnp.sum(products * conduction_panel[None], axis=2))
    potential = jnp.einsum('mn,kn->km', bare_coulomb, density, precision=precise)
    weighted = potential[:, :, None] * conduction_panel[None]
    exchange = jnp.einsum('mv,kmc->kvc', valence_panel, weighted, precision=precise)
    pair_amp = jnp.einsum('mc,kvc->kmv', conduction_panel, lanczos_now, precision=precise)
    block_size = min(512, NP)
    block_count = NP // block_size

    def one_block(index, total):
        first_row = (index * block_size).astype(jnp.int32)
        pair_rows = lax.dynamic_slice_in_dim(pair_amp, first_row, block_size, 1)
        kernel_rows = lax.dynamic_slice_in_dim(screened_coulomb, first_row, block_size, 0)
        cond_rows = lax.dynamic_slice_in_dim(conduction_panel, first_row, block_size, 0)
        pair_terms = jnp.einsum('kmv,nv->kmn', pair_rows, valence_panel, precision=precise) * kernel_rows[None]
        screened = jnp.einsum('kmn,nv->kmv', pair_terms, valence_panel, precision=precise)
        return total + jnp.einsum('kmv,mc->kvc', screened, cond_rows, precision=precise)
    direct = lax.fori_loop(0, block_count, one_block, jnp.zeros((NVEC, V, C), jnp.float32))
    gaps = conduction_energy[None, None, :] - valence_energy[None, :, None]
    image = gaps * lanczos_now + 2.0 * exchange - direct
    coef_alpha = lax.optimization_barrier(jnp.mean(lanczos_now * image, axis=(1, 2))) / (lax.optimization_barrier(jnp.mean(lanczos_now * lanczos_now, axis=(1, 2))) + epsilon)
    resid = image - coef_alpha[:, None, None] * lanczos_now - beta_prev[:, None, None] * lanczos_prev
    beta_next = jnp.sqrt(lax.optimization_barrier(jnp.mean(resid * resid, axis=(1, 2))) + epsilon)
    return (resid / beta_next[:, None, None], jnp.stack([coef_alpha, beta_next], axis=1))
```

```python
import jax
import jax.numpy as jnp
from jax import lax
from jax.sharding import Mesh
from jax.sharding import PartitionSpec as P

V = 256
C = 1024
X, H, Y, L, K = "row_0", "row_1", "row_2", "col_0", "col_1"
SIZES = (4, 2, 4, 4, 2)
AXES = (X, H, Y, L, K)
ROW = (X, H, Y)
COL = (L, K)

split = lax.Precision.HIGH
epsilon = 1e-06
middle_gap = 2.5


def from_all(block, axes):
    copies = jnp.broadcast_to(block, (lax.axis_size(axes), *block.shape))
    return lax.all_to_all(copies, axes, split_axis=0, concat_axis=0, tiled=True)


def from_partner(block):
    return lax.ppermute(block, K, [(0, 1), (1, 0)])


def by_core(own, other, dim):
    south = lax.axis_index(K) == 0
    return jnp.stack([jnp.where(south, own, other), jnp.where(south, other, own)], axis=dim)


def grid_swap(block, flip):
    pairs = []
    for a in range(4):
        for b in range(2):
            for c in range(4):
                for d in range(4):
                    for e in range(2):
                        source = (((a * 2 + b) * 4 + c) * 4 + d) * 2 + e
                        e2 = e ^ flip
                        target = (((d * 2 + e2) * 4 + c) * 4 + a) * 2 + b
                        pairs.append((source, target))
    return lax.ppermute(block, AXES, pairs)


def per_device(q, p, beta_prev, ev, ec, pv, pc, screened_coulomb, bare_coulomb):
    core = lax.axis_index(K)
    q, p = q[0], p[0]
    first, second = grid_swap(pv, 0), grid_swap(pv, 1)
    low = lax.axis_index(H) == 0
    panel_pair = jnp.stack([jnp.where(low, first, second), jnp.where(low, second, first)])
    panel = from_all(panel_pair, (Y, X)).reshape(2048, V)

    gap_q = (ec[None, :] - ev[:, None]) * q
    piece = from_all(jnp.stack([q, p, gap_q]), (H, L))
    q_piece, p_piece, gap_piece = piece[:, 0], piece[:, 1], piece[:, 2]
    own_half = from_all(q_piece, (X, Y)).reshape(4, 4, 2, 4, 8, 128)
    other_half = from_partner(own_half)

    def as_matrix(half):
        return jnp.transpose(half, (0, 2, 1, 4, 3, 5)).reshape(V, C // 2)

    pc4 = pc.reshape(64, 4, 2, 128)
    pc_own = lax.dynamic_index_in_dim(pc4, core, 2, False).reshape(64, C // 2)
    pc_other = lax.dynamic_index_in_dim(pc4, 1 - core, 2, False).reshape(64, C // 2)
    pair_local = jnp.einsum("pc,vc->pv", pc_own, as_matrix(own_half), precision=split)
    pair_local += jnp.einsum("pc,vc->pv", pc_other, as_matrix(other_half), precision=split)
    density = jnp.sum(pair_local * pv, axis=1)

    density_row = jnp.pad(density[None, :], ((0, 7), (0, V - 64)))
    both = jnp.concatenate([pair_local, density_row], axis=0)
    own = from_all(both, L)
    rows = by_core(own, from_partner(own), 1)
    pair_rows = rows[:, :, :64].reshape(512, V)
    row_density = rows[:, :, 64, :64].reshape(4, 128)
    far_density = from_all(grid_swap(row_density, 0), Y).reshape(2048)

    terms = jnp.einsum("mv,nv->mn", pair_rows, panel, precision=split) * screened_coulomb
    screened = jnp.einsum("mn,nv->mv", terms, panel, precision=split)
    potential = jnp.einsum("mn,n->m", bare_coulomb, far_density, precision=lax.Precision.HIGHEST)
    potential = jnp.pad(potential.reshape(4, 2, 1, 64), ((0, 0), (0, 0), (0, 7), (0, V - 64)))
    parts = jnp.concatenate([screened.reshape(4, 2, 64, V), potential], axis=2)
    mine = lax.dynamic_index_in_dim(parts, core, 1, False)
    theirs = lax.dynamic_index_in_dim(parts, 1 - core, 1, False)
    mine += from_partner(theirs)
    done = lax.all_to_all(mine, L, split_axis=0, concat_axis=0, tiled=True).sum(axis=0)
    source = 2.0 * done[64, :64][:, None] * pv - done[:64]

    theirs = jnp.einsum("pv,pc->vc", source, pc_other, precision=split)
    total = jnp.einsum("pv,pc->vc", source, pc_own, precision=split) + from_partner(theirs)
    total = jnp.transpose(total.reshape(4, 2, 4, 8, 4, 128), (0, 2, 1, 4, 3, 5))
    total = total.reshape(16, 8, 8, 128)
    total = lax.all_to_all(total, (X, Y), split_axis=0, concat_axis=0, tiled=True).sum(axis=0)
    kernel_piece = from_all(total, (H, L)).sum(axis=0)

    shifted = gap_piece + kernel_piece - middle_gap * q_piece - beta_prev[0] * p_piece
    sums = jnp.stack(
        [
            jnp.sum(shifted * shifted),
            jnp.sum(shifted * q_piece),
            jnp.sum(q_piece * q_piece),
            jnp.sum(q_piece * p_piece),
        ]
    )
    sums = jnp.pad(sums, (0, 4))[None, :]
    sums = from_all(sums, (X, Y, K)).sum(axis=(0, 1)) * (1.0 / (V * C))
    mean_ww, mean_wq, mean_qq, mean_qp = sums[0], sums[1], sums[2], sums[3]
    mean_qu = mean_wq + middle_gap * mean_qq + beta_prev[0] * mean_qp
    alpha = mean_qu / (mean_qq + epsilon)
    rest = alpha - middle_gap
    mean_rr = mean_ww - 2.0 * rest * mean_wq + rest * rest * mean_qq
    beta = jnp.sqrt(mean_rr + epsilon)
    at = lax.axis_index((H, L))
    own_shifted = lax.dynamic_index_in_dim(shifted, at, 0, False)
    following = (own_shifted - rest * q) / beta
    return following[None], jnp.stack([alpha, beta])[None, :]


def solution(mesh):
    torus = Mesh(mesh.devices.reshape(SIZES), AXES)
    return jax.shard_map(
        per_device,
        mesh=torus,
        in_specs=(
            P(None, ROW, COL),
            P(None, ROW, COL),
            P(),
            P(ROW),
            P(COL),
            P(AXES, None),
            P(AXES, None),
            P(ROW, COL),
            P(ROW, COL),
        ),
        out_specs=(P(None, ROW, COL), P()),
        check_vma=False,
    )
```

```python
import jax
import jax.numpy as jnp
from jax import lax
from jax.sharding import Mesh
from jax.sharding import PartitionSpec as P

V = 256
C = 1024
X, H, Y, L, K = "row_0", "row_1", "row_2", "col_0", "col_1"
SIZES = (4, 2, 4, 4, 2)
AXES = (X, H, Y, L, K)
ROW = (X, H, Y)
COL = (L, K)

split = lax.Precision.HIGH
epsilon = 1e-06
middle_gap = 2.5


def from_all(block, axes):
    copies = jnp.broadcast_to(block, (lax.axis_size(axes), *block.shape))
    return lax.all_to_all(copies, axes, split_axis=0, concat_axis=0, tiled=True)


def from_partner(block):
    return lax.ppermute(block, K, [(0, 1), (1, 0)])


def by_core(own, other, dim):
    south = lax.axis_index(K) == 0
    return jnp.stack([jnp.where(south, own, other), jnp.where(south, other, own)], axis=dim)


def from_next(block, shift):
    return lax.ppermute(block, L, [((i + shift) % 4, i) for i in range(4)])


def from_own(blocks):
    twice = jnp.concatenate([blocks, blocks[:3]])
    return lax.dynamic_slice_in_dim(twice, lax.axis_index(L), 4, 0)


def grid_swap(block, flip):
    pairs = []
    for a in range(4):
        for b in range(2):
            for c in range(4):
                for d in range(4):
                    for e in range(2):
                        source = (((a * 2 + b) * 4 + c) * 4 + d) * 2 + e
                        e2 = e ^ flip
                        target = (((d * 2 + e2) * 4 + c) * 4 + a) * 2 + b
                        pairs.append((source, target))
    return lax.ppermute(block, AXES, pairs)


def per_device(q, p, beta_prev, ev, ec, pv, pc, screened_coulomb, bare_coulomb):
    core = lax.axis_index(K)
    q, p = q[0], p[0]
    first = grid_swap(pv, 0)
    second = grid_swap(pv, 1)
    gap_q = (ec[None, :] - ev[:, None]) * q
    piece = from_all(jnp.stack([q, p, gap_q]), (H, L))
    q_piece, p_piece, gap_piece = piece[:, 0], piece[:, 1], piece[:, 2]
    low = lax.axis_index(H) == 0
    panel_pair = jnp.concatenate([jnp.where(low, first, second), jnp.where(low, second, first)])
    sent = jnp.concatenate([panel_pair.reshape(32, 8, 128), q_piece])
    points = lax.optimization_barrier(jnp.concatenate([pv, pc], axis=1))
    points_1 = from_next(points, 1)
    points_2 = from_next(points, 2)
    points_3 = from_next(points, 3)
    arrived = from_all(sent, (Y, X))
    panel = arrived[:, :32].reshape(2048, V)
    own_half = arrived[:, 32:].reshape(4, 4, 2, 4, 8, 128)
    own_points = jnp.concatenate([points, points_1, points_2, points_3])
    other_half = from_partner(own_half)
    other_points = from_partner(own_points)

    def as_matrix(half):
        return jnp.transpose(half, (1, 2, 0, 4, 3, 5)).reshape(V, C // 2)

    pc4 = pc.reshape(64, 4, 2, 128)
    pc_own = lax.dynamic_index_in_dim(pc4, core, 2, False).reshape(64, C // 2)
    pc_other = lax.dynamic_index_in_dim(pc4, 1 - core, 2, False).reshape(64, C // 2)
    pair_local = jnp.einsum("pc,vc->pv", pc_own, as_matrix(own_half), precision=split)
    pair_local += jnp.einsum("pc,vc->pv", pc_other, as_matrix(other_half), precision=split)
    density = jnp.sum(pair_local * pv, axis=1)

    density_row = jnp.pad(density[None, :], ((0, 7), (0, V - 64)))
    both = jnp.concatenate([pair_local, density_row], axis=0)
    own = from_all(both, L)
    rows = by_core(own, from_partner(own), 1)
    pair_rows = rows[:, :, :64].reshape(512, V)
    row_density = rows[:, :, 64, :64].reshape(4, 128)
    swapped = grid_swap(row_density, 0)
    far_density = from_all(swapped, Y).reshape(2048)

    terms = jnp.einsum("mv,nv->mn", pair_rows, panel, precision=split) * screened_coulomb
    screened = jnp.einsum("mn,nv->mv", terms, panel, precision=split)
    potential = jnp.einsum("mn,n->m", bare_coulomb, far_density, precision=lax.Precision.HIGHEST)
    screened = from_own(screened.reshape(4, 2, 64, V))
    potential = from_own(potential.reshape(4, 2, 64))

    def at_core(which, there):
        rows = lax.dynamic_index_in_dim(screened, which, 1, False).reshape(256, V)
        at = lax.dynamic_index_in_dim(potential, which, 1, False).reshape(256, 1)
        return 2.0 * at * there[:, :V] - rows

    source = jnp.concatenate([at_core(core, own_points), at_core(1 - core, other_points)])
    at_points = jnp.concatenate([own_points[:, V:], other_points[:, V:]]).reshape(512, 4, 2, 128)

    def from_points(which):
        columns = lax.dynamic_index_in_dim(at_points, which, 2, False).reshape(512, C // 2)
        return jnp.einsum("pv,pc->vc", source, columns, precision=split)

    total = from_partner(from_points(1 - core)) + from_points(core)
    total = jnp.transpose(total.reshape(4, 2, 4, 8, 4, 128), (0, 2, 1, 4, 3, 5))
    total = total.reshape(16, 8, 8, 128)
    total = lax.all_to_all(total, (X, Y), split_axis=0, concat_axis=0, tiled=True).sum(axis=0)
    kernel_piece = from_all(total, (H, L)).sum(axis=0)

    shifted = gap_piece + kernel_piece - middle_gap * q_piece - beta_prev[0] * p_piece
    sums = jnp.stack(
        [
            jnp.sum(shifted * shifted),
            jnp.sum(shifted * q_piece),
            jnp.sum(q_piece * q_piece),
            jnp.sum(q_piece * p_piece),
        ]
    )
    sums = jnp.pad(sums, (0, 4))[None, :]
    sums = from_all(sums, (X, Y, K)).sum(axis=(0, 1)) * (1.0 / (V * C))
    mean_ww, mean_wq, mean_qq, mean_qp = sums[0], sums[1], sums[2], sums[3]
    mean_qu = mean_wq + middle_gap * mean_qq + beta_prev[0] * mean_qp
    alpha = mean_qu / (mean_qq + epsilon)
    rest = alpha - middle_gap
    mean_rr = mean_ww - 2.0 * rest * mean_wq + rest * rest * mean_qq
    beta = jnp.sqrt(mean_rr + epsilon)
    at = lax.axis_index((H, L))
    own_shifted = lax.dynamic_index_in_dim(shifted, at, 0, False)
    following = (own_shifted - rest * q) / beta
    return following[None], jnp.stack([alpha, beta])[None, :]


def solution(mesh):
    torus = Mesh(mesh.devices.reshape(SIZES), AXES)
    return jax.shard_map(
        per_device,
        mesh=torus,
        in_specs=(
            P(None, ROW, COL),
            P(None, ROW, COL),
            P(),
            P(ROW),
            P(COL),
            P(AXES, None),
            P(AXES, None),
            P(ROW, COL),
            P(ROW, COL),
        ),
        out_specs=(P(None, ROW, COL), P()),
        check_vma=False,
    )
```

```python
import jax
import jax.numpy as jnp
from jax import lax
from jax.experimental import pallas as pl
from jax.experimental.pallas import tpu as pltpu
from jax.sharding import Mesh
from jax.sharding import PartitionSpec as P

V = 256
C = 1024
X, H, Y, L, K = "row_0", "row_1", "row_2", "col_0", "col_1"
SIZES = (4, 2, 4, 4, 2)
AXES = (X, H, Y, L, K)
ROW = (X, H, Y)
COL = (L, K)

f32 = jnp.float32
bf16 = jnp.bfloat16
epsilon = 1e-06
middle_gap = 2.5
inverse_size = 1.0 / (V * C)
SMEM = pl.BlockSpec(memory_space=pltpu.SMEM)
VMEM = pl.BlockSpec(memory_space=pltpu.VMEM)


def copies_to_all(copies, axes):
    return lax.all_to_all(copies, axes, split_axis=0, concat_axis=0, tiled=True)


def from_all(block, axes):
    return copies_to_all(jnp.broadcast_to(block, (lax.axis_size(axes), *block.shape)), axes)


def from_partner(block):
    return lax.ppermute(block, K, [(0, 1), (1, 0)])


def from_next(block, axis, shift):
    return lax.ppermute(block, axis, [((i + shift) % 4, i) for i in range(4)])


def grid_swap(block, flip):
    pairs = []
    for a in range(4):
        for b in range(2):
            for c in range(4):
                for d in range(4):
                    for e in range(2):
                        source = (((a * 2 + b) * 4 + c) * 4 + d) * 2 + e
                        target = (((d * 2 + (e ^ flip)) * 4 + c) * 4 + a) * 2 + b
                        pairs.append((source, target))
    return lax.ppermute(block, AXES, pairs)


def iota(shape, dim):
    return lax.broadcasted_iota(jnp.int32, shape, dim)


def halves(a):
    high = a.astype(bf16)
    return high, (a - high.astype(f32)).astype(bf16)


def product(a, b, dims):
    def one(x, y):
        return lax.dot_general(x, y, (dims, ((), ())), preferred_element_type=f32)

    return one(a[0], b[0]) + (one(a[0], b[1]) + one(a[1], b[0]))


ROWS_BY_ROWS = ((1,), (1,))
PLAIN = ((1,), (0,))
COLUMNS_BY_COLUMNS = ((0,), (0,))


def local_kernel(body, out, flops, scratch=(), grant=8):
    shapes = [pltpu.VMEM(s, f32) for s in out]
    many = len(shapes) > 1

    def call(*args, arguments=()):
        placed = [
            a if a.ndim == 1 else pltpu.with_memory_space_constraint(a, pltpu.VMEM) for a in args
        ] + list(arguments)
        specs = [SMEM if a.ndim == 1 else VMEM for a in placed]
        return pl.pallas_call(
            body,
            out_shape=shapes if many else shapes[0],
            in_specs=specs,
            out_specs=[VMEM] * len(shapes) if many else VMEM,
            scratch_shapes=list(scratch),
            compiler_params=pltpu.CompilerParams(vmem_limit_bytes=grant << 20),
            cost_estimate=pl.CostEstimate(flops=flops, bytes_accessed=1 << 20, transcendentals=0),
        )(*placed)

    return call


def as_column(row, count):
    square = jnp.broadcast_to(row[:, :count], (count, count))
    same = iota((count, count), 0) == iota((count, count), 1)
    return jnp.sum(jnp.where(same, square, 0.0), axis=1, keepdims=True)


def as_row(column, count):
    wide = jnp.broadcast_to(column, (count, V))
    same = iota((count, V), 0) == iota((count, V), 1)
    return jnp.sum(jnp.where(same, wide, 0.0), axis=0, keepdims=True)


def first_kernel(ev_ref, q_ref, p_ref, ec_ref, out_ref):
    ev = jnp.zeros((8, 128), f32)
    for i in range(8):
        ev = jnp.where(iota((8, 128), 0) == i, ev_ref[i], ev)
    gap_q = (ec_ref[...] - ev) * q_ref[...]
    for n in range(8):
        out_ref[n, 0] = q_ref[...]
        out_ref[n, 1] = p_ref[...]
        out_ref[n, 2] = gap_q


def columns_of(pc_ref, which):
    parts = [pc_ref[:, pl.ds(pl.multiple_of((2 * l + which) * 128, 128), 128)] for l in range(4)]
    return halves(jnp.concatenate(parts, axis=1))


def amplitude_kernel(at_ref, own_ref, other_ref, pc_ref, pv_ref, out_ref):
    core = at_ref[0]
    total = jnp.zeros((64, V), f32)
    for ref, which in ((own_ref, core), (other_ref, 1 - core)):
        columns = [
            jnp.concatenate(
                [ref[x * 4 + y, h * 4 + l] for x in range(4) for h in range(2) for y in range(4)],
                axis=0,
            )
            for l in range(4)
        ]
        vectors = halves(jnp.concatenate(columns, axis=1))
        total += product(columns_of(pc_ref, which), vectors, ROWS_BY_ROWS)
    density = as_row(jnp.sum(total * pv_ref[...], axis=1, keepdims=True), 64)
    tail = jnp.where(iota((8, V), 0) == 0, jnp.broadcast_to(density, (8, V)), 0.0)
    for n in range(4):
        out_ref[n, :64] = total
        out_ref[n, 64:] = tail


def density_kernel(at_ref, own_ref, other_ref, out_ref):
    south = at_ref[0] == 0
    for l in range(4):
        own, other = own_ref[l, 64:65, :128], other_ref[l, 64:65, :128]
        first, second = jnp.where(south, own, other), jnp.where(south, other, own)
        out_ref[l : l + 1, :] = first + pltpu.roll(second, 64, 1)


def screened_kernel(at_ref, own_ref, other_ref, *refs):
    a_refs, b_refs, (w_ref, mine_ref, theirs_ref, terms_ref) = refs[:4], refs[4:8], refs[8:]
    core, x, y = at_ref[0], at_ref[1], at_ref[2]
    sides = ((own_ref, core, mine_ref), (other_ref, 1 - core, theirs_ref))
    pairs = [halves(jnp.concatenate([r[l, :64] for l in range(4)], axis=0)) for r, _, _ in sides]
    for t in range(4):
        points = [piece for s in range(4) for piece in (a_refs[t][s], b_refs[s][t])]
        points = halves(jnp.concatenate(points, axis=0))
        for (_, which, out_ref), pair in zip(sides, pairs):
            terms_ref[...] = product(pair, points, ROWS_BY_ROWS)
            for s in range(4):
                at = lax.rem(y + s, 4) * 512 + lax.rem(x + t, 4) * 128
                for l in range(4):
                    rows = pl.ds(pl.multiple_of((2 * l + which) * 64, 64), 64)
                    tile = w_ref[rows, pl.ds(pl.multiple_of(at, 128), 128)]
                    here = (slice(l * 64, l * 64 + 64), slice(s * 128, s * 128 + 128))
                    terms_ref[here] = terms_ref[here] * tile
            done = product(halves(terms_ref[...]), points, PLAIN)
            done = done.reshape(4, 64, V)
            out_ref[...] = done if t == 0 else out_ref[...] + done


def bare_kernel(at_ref, density_ref, b_ref, mine_ref, theirs_ref):
    south = at_ref[0] == 0
    for l in range(4):
        rows = slice(l * 128, l * 128 + 128)
        total = jnp.zeros((128, 128), f32)
        for n in range(16):
            total += b_ref[rows, n * 128 : n * 128 + 128] * density_ref[n : n + 1, :]
        line = jnp.sum(total.T, axis=0, keepdims=True)
        first = jnp.concatenate([line, line], axis=1)
        second = pltpu.roll(first, 192, 1)
        keep = (iota((8, V), 0) == 0) & (iota((8, V), 1) < 64)
        first = jnp.where(keep, jnp.broadcast_to(first, (8, V)), 0.0)
        second = jnp.where(keep, jnp.broadcast_to(second, (8, V)), 0.0)
        mine_ref[l] = jnp.where(south, first, second)
        theirs_ref[l] = jnp.where(south, second, first)


def contribution_kernel(at_ref, sums_ref, pv_ref, pc_ref, own_ref, other_ref):
    core = at_ref[0]
    total = (sums_ref[0] + sums_ref[1]) + (sums_ref[2] + sums_ref[3])
    potential = as_column(total[64:65], 64)
    source = halves(2.0 * potential * pv_ref[...] - total[:64])
    for ref, which in ((other_ref, 1 - core), (own_ref, core)):
        done = product(source, columns_of(pc_ref, which), COLUMNS_BY_COLUMNS)
        for x in range(4):
            for h in range(2):
                for y in range(4):
                    v = ((x * 2 + h) * 4 + y) * 8
                    for l in range(4):
                        ref[x * 4 + y, h * 4 + l] = done[v : v + 8, l * 128 : l * 128 + 128]


def plane_sum_kernel(parts_ref, out_ref):
    for n in range(8):
        total = parts_ref[0, n]
        for i in range(1, 16):
            total += parts_ref[i, n]
        for i in range(8):
            out_ref[i, n] = total


def total_of(a):
    return jnp.sum(jnp.sum(a, axis=0, keepdims=True), axis=1, keepdims=True)


def sums_kernel(beta_ref, parts_ref, piece_ref, shifted_ref, sums_ref):
    beta_prev = beta_ref[0]
    sums = [jnp.zeros((8, 128), f32) for _ in range(4)]
    for n in range(8):
        total = parts_ref[0, n]
        for i in range(1, 8):
            total += parts_ref[i, n]
        q, p = piece_ref[n, 0], piece_ref[n, 1]
        shifted = piece_ref[n, 2] + total - middle_gap * q - beta_prev * p
        shifted_ref[n] = shifted
        sums = [sums[0] + shifted * shifted, sums[1] + shifted * q, sums[2] + q * q, sums[3] + q * p]
    line = jnp.zeros((1, 128), f32)
    for i in range(4):
        line = jnp.where(iota((1, 128), 1) == i, total_of(sums[i]), line)
    for i in range(32):
        sums_ref[i] = line


def last_kernel(beta_ref, at_ref, sums_ref, shifted_ref, q_ref, out_ref, coefficient_ref):
    line = sums_ref[0]
    for i in range(1, 32):
        line += sums_ref[i]
    line = line * inverse_size
    lane = iota((1, 128), 1)
    mean_ww, mean_wq, mean_qq, mean_qp = (
        jnp.sum(jnp.where(lane == i, line, 0.0), axis=1, keepdims=True) for i in range(4)
    )
    mean_qu = mean_wq + middle_gap * mean_qq + beta_ref[0] * mean_qp
    alpha = mean_qu / (mean_qq + epsilon)
    rest = alpha - middle_gap
    mean_rr = mean_ww - 2.0 * rest * mean_wq + rest * rest * mean_qq
    beta = jnp.sqrt(mean_rr + epsilon)
    shifted = shifted_ref[at_ref[3]]
    out_ref[...] = (shifted - rest * q_ref[...]) / beta
    coefficient_ref[...] = jnp.where(iota((1, 2), 1) == 0, alpha, beta)


def per_device(q, p, beta_prev, ev, ec, pv, pc, screened_coulomb, bare_coulomb):
    at = jnp.stack([lax.axis_index(K), lax.axis_index(X), lax.axis_index(Y), lax.axis_index((H, L))])
    at = at.astype(jnp.int32)
    q, p = q[0], p[0]
    copies = local_kernel(first_kernel, [(8, 3, 8, 128)], 1 << 16)(
        arguments=(ev, q, p, ec[None, :])
    )
    piece = copies_to_all(copies, (H, L))
    own_half = from_all(piece[:, 0], (X, Y))
    other_half = from_partner(own_half)

    first, second = grid_swap(pv, 0), grid_swap(pv, 1)
    low = lax.axis_index(H) == 0
    a, b = jnp.where(low, first, second), jnp.where(low, second, first)
    a_parts = jnp.stack([a] + [from_next(a, Y, s) for s in (1, 2, 3)])
    b_parts = jnp.stack([b] + [from_next(b, X, s) for s in (1, 2, 3)])
    a_parts = [a_parts] + [from_next(a_parts, X, s) for s in (1, 2, 3)]
    b_parts = [b_parts] + [from_next(b_parts, Y, s) for s in (1, 2, 3)]

    copies = local_kernel(amplitude_kernel, [(4, 72, V)], 1 << 27)(
        at, own_half, other_half, arguments=(pc, pv)
    )
    own_rows = copies_to_all(copies, L)
    other_rows = from_partner(own_rows)
    row_density = local_kernel(density_kernel, [(4, 128)], 1 << 10)(at, own_rows, other_rows)
    swapped = grid_swap(row_density, 0)
    far_density = from_all(swapped, Y).reshape(16, 128)

    mine, theirs = local_kernel(
        screened_kernel, [(4, 64, V), (4, 64, V)], 3 << 30, [pltpu.VMEM((256, 512), f32)], 24
    )(at, own_rows, other_rows, *a_parts, *b_parts, arguments=(screened_coulomb,))
    mine += from_partner(theirs)
    potential, their_potential = local_kernel(
        bare_kernel, [(4, 8, V), (4, 8, V)], 1 << 26, grant=12
    )(at, far_density, arguments=(bare_coulomb,))
    potential += from_partner(their_potential)
    sums = copies_to_all(jnp.concatenate([mine, potential], axis=1), L)

    own_half, other_half = local_kernel(
        contribution_kernel, [(16, 8, 8, 128)] * 2, 1 << 28
    )(at, sums, arguments=(pv, pc))
    own_half += from_partner(other_half)
    parts = copies_to_all(own_half, (X, Y))
    copies = local_kernel(plane_sum_kernel, [(8, 8, 8, 128)], 1 << 18)(parts)
    parts = copies_to_all(copies, (H, L))

    shifted, sums = local_kernel(
        sums_kernel, [(8, 8, 128), (32, 1, 128)], 1 << 18
    )(beta_prev, parts, piece)
    sums = copies_to_all(sums, (X, Y, K))
    following, coefficients = local_kernel(
        last_kernel, [(8, 128), (1, 2)], 1 << 16
    )(beta_prev, at, sums, shifted, arguments=(q,))
    return following[None], coefficients


def solution(mesh):
    torus = Mesh(mesh.devices.reshape(SIZES), AXES)
    return jax.shard_map(
        per_device,
        mesh=torus,
        in_specs=(
            P(None, ROW, COL),
            P(None, ROW, COL),
            P(),
            P(ROW),
            P(COL),
            P(AXES, None),
            P(AXES, None),
            P(ROW, COL),
            P(ROW, COL),
        ),
        out_specs=(P(None, ROW, COL), P()),
        check_vma=False,
    )
```

```python
import functools

import jax
import jax.numpy as jnp
from jax import lax
from jax.experimental import pallas as pl
from jax.experimental.pallas import tpu as pltpu
from jax.sharding import Mesh
from jax.sharding import PartitionSpec as P

V = 256
C = 1024
X, H, Y, L, K = "row_0", "row_1", "row_2", "col_0", "col_1"
SIZES = (4, 2, 4, 4, 2)
AXES = (X, H, Y, L, K)
ROW = (X, H, Y)
COL = (L, K)

f32 = jnp.float32
bf16 = jnp.bfloat16
epsilon = 1e-06
middle_gap = 2.5
inverse_size = 1.0 / (V * C)
SMEM = pl.BlockSpec(memory_space=pltpu.SMEM)
VMEM = pl.BlockSpec(memory_space=pltpu.VMEM)
HBM = pl.BlockSpec(memory_space=pltpu.HBM)


def copies_to_all(copies, axes):
    return lax.all_to_all(copies, axes, split_axis=0, concat_axis=0, tiled=True)


def from_all(block, axes):
    return copies_to_all(jnp.broadcast_to(block, (lax.axis_size(axes), *block.shape)), axes)


def from_partner(block):
    return lax.ppermute(block, K, [(0, 1), (1, 0)])


def from_next(block, axis, shift):
    return lax.ppermute(block, axis, [((i + shift) % 4, i) for i in range(4)])


def grid_swap(block, flip):
    pairs = []
    for a in range(4):
        for b in range(2):
            for c in range(4):
                for d in range(4):
                    for e in range(2):
                        source = (((a * 2 + b) * 4 + c) * 4 + d) * 2 + e
                        target = (((d * 2 + (e ^ flip)) * 4 + c) * 4 + a) * 2 + b
                        pairs.append((source, target))
    return lax.ppermute(block, AXES, pairs)


def iota(shape, dim):
    return lax.broadcasted_iota(jnp.int32, shape, dim)


def halves(a):
    high = a.astype(bf16)
    return high, (a - high.astype(f32)).astype(bf16)


def product(a, b, dims):
    def one(x, y):
        return lax.dot_general(x, y, (dims, ((), ())), preferred_element_type=f32)

    return one(a[0], b[0]) + (one(a[0], b[1]) + one(a[1], b[0]))


ROWS_BY_ROWS = ((1,), (1,))
PLAIN = ((1,), (0,))
COLUMNS_BY_COLUMNS = ((0,), (0,))


def local_kernel(body, out, flops, scratch=(), grant=8, placed=True):
    shapes = [pltpu.VMEM(s, f32) if placed else jax.ShapeDtypeStruct(s, f32) for s in out]
    many = len(shapes) > 1

    def call(*args, arguments=(), far=()):
        near = [
            a if a.ndim == 1 else pltpu.with_memory_space_constraint(a, pltpu.VMEM) for a in args
        ]
        near += list(arguments)
        far = [pltpu.with_memory_space_constraint(a, pltpu.HBM) for a in far]
        specs = [SMEM if a.ndim == 1 else VMEM for a in near] + [HBM] * len(far)
        return pl.pallas_call(
            body,
            out_shape=shapes if many else shapes[0],
            in_specs=specs,
            out_specs=[VMEM] * len(shapes) if many else VMEM,
            scratch_shapes=list(scratch),
            compiler_params=pltpu.CompilerParams(vmem_limit_bytes=grant << 20),
            cost_estimate=pl.CostEstimate(flops=flops, bytes_accessed=1 << 20, transcendentals=0),
        )(*near, *far)

    return call


def as_row(column, count):
    wide = jnp.broadcast_to(column, (count, V))
    same = iota((count, V), 0) == iota((count, V), 1)
    return jnp.sum(jnp.where(same, wide, 0.0), axis=0, keepdims=True)


def first_kernel(
    ev_ref, q_hbm, p_hbm, ec_hbm, pv_hbm, pc_hbm, out_ref, points_ref, q_ref, p_ref, ec_ref, sems
):
    pieces = (
        (q_hbm, q_ref),
        (p_hbm, p_ref),
        (ec_hbm, ec_ref),
        (pv_hbm, points_ref.at[:, :V]),
        (pc_hbm, points_ref.at[:, V:]),
    )
    moves = [pltpu.make_async_copy(a, b, sems.at[n]) for n, (a, b) in enumerate(pieces)]
    for move in moves:
        move.start()
    ev = jnp.zeros((8, 128), f32)
    for i in range(8):
        ev = jnp.where(iota((8, 128), 0) == i, ev_ref[i], ev)
    for move in moves[:3]:
        move.wait()
    gap_q = (ec_ref[...] - ev) * q_ref[...]
    for n in range(8):
        out_ref[n, 0] = q_ref[...]
        out_ref[n, 1] = p_ref[...]
        out_ref[n, 2] = gap_q
    for move in moves[3:]:
        move.wait()


def choose_kernel(at_ref, first_ref, second_ref, a_ref, b_ref):
    low = at_ref[5] == 0
    a_ref[...] = jnp.where(low, first_ref[...], second_ref[...])
    b_ref[...] = jnp.where(low, second_ref[...], first_ref[...])


def columns_of(points_ref, which):
    parts = [
        points_ref[:, pl.ds(pl.multiple_of(V + (2 * l + which) * 128, 128), 128)] for l in range(4)
    ]
    return jnp.concatenate(parts, axis=1)


def amplitude_kernel(at_ref, own_ref, other_ref, points_ref, out_ref):
    core = at_ref[0]
    total = jnp.zeros((64, V), f32)
    for ref, which in ((own_ref, core), (other_ref, 1 - core)):
        columns = [
            jnp.concatenate(
                [ref[x * 4 + y, h * 4 + l] for x in range(4) for h in range(2) for y in range(4)],
                axis=0,
            )
            for l in range(4)
        ]
        vectors = halves(jnp.concatenate(columns, axis=1))
        total += product(halves(columns_of(points_ref, which)), vectors, ROWS_BY_ROWS)
    density = as_row(jnp.sum(total * points_ref[:, :V], axis=1, keepdims=True), 64)
    tail = jnp.where(iota((8, V), 0) == 0, jnp.broadcast_to(density, (8, V)), 0.0)
    for n in range(4):
        out_ref[n, :64] = total
        out_ref[n, 64:] = tail


def density_kernel(at_ref, own_ref, other_ref, out_ref):
    south = at_ref[0] == 0
    for l in range(4):
        own, other = own_ref[l, 64:65, :128], other_ref[l, 64:65, :128]
        first, second = jnp.where(south, own, other), jnp.where(south, other, own)
        out_ref[l : l + 1, :] = first + pltpu.roll(second, 64, 1)


def screened_kernel(turns, at_ref, own_ref, other_ref, *refs):
    a_refs, b_refs, refs = refs[:4], refs[4:8], refs[8:]
    so_far_ref = None
    if turns[0] > 0:
        so_far_ref, refs = refs[0], refs[1:]
    core, x, y = at_ref[0], at_ref[1], at_ref[2]
    w_hbm, out_ref, w_ref, terms_ref, sems = refs
    moves = []
    for n, t in enumerate(turns):
        for s in range(4):
            at = pl.multiple_of(lax.rem(y + s, 4) * 512 + lax.rem(x + t, 4) * 128, 128)
            moves.append(
                pltpu.make_async_copy(
                    w_hbm.at[:, pl.ds(at, 128)], w_ref.at[n * 4 + s], sems.at[n * 4 + s]
                )
            )
            moves[-1].start()
    pairs = [
        halves(jnp.concatenate([r[l, :64] for l in range(4)], axis=0)) for r in (own_ref, other_ref)
    ]
    for n, t in enumerate(turns):
        points = [piece for s in range(4) for piece in (a_refs[t][s], b_refs[s][t])]
        points = halves(jnp.concatenate(points, axis=0))
        for side, which in enumerate((core, 1 - core)):
            terms_ref[...] = product(pairs[side], points, ROWS_BY_ROWS)
            for s in range(4):
                if side == 0:
                    moves[n * 4 + s].wait()
                for l in range(4):
                    rows = pl.ds(pl.multiple_of((2 * l + which) * 64, 64), 64)
                    here = (slice(l * 64, l * 64 + 64), slice(s * 128, s * 128 + 128))
                    terms_ref[here] = terms_ref[here] * w_ref[n * 4 + s, rows, :]
            done = product(halves(terms_ref[...]), points, PLAIN)
            mine = slice(side * 256, side * 256 + 256)
            if n > 0:
                done += out_ref[mine]
            elif so_far_ref is not None:
                done += so_far_ref[mine]
            out_ref[mine] = done


def contribution_kernel(at_ref, density_ref, screened_ref, *refs):
    points_refs, (b_hbm, own_ref, other_ref, b_ref, sems) = refs[:8], refs[8:]
    core, z = at_ref[0], at_ref[4]
    moves = []
    for side, which in enumerate((core, 1 - core)):
        for s in range(4):
            at = pl.multiple_of((2 * lax.rem(z + s, 4) + which) * 64, 64)
            n = side * 4 + s
            moves.append(
                pltpu.make_async_copy(b_hbm.at[pl.ds(at, 64), :], b_ref.at[n], sems.at[n])
            )
            moves[-1].start()
    source = []
    for side in range(2):
        for s in range(4):
            l = lax.rem(z + s, 4)
            total = jnp.zeros((64, 128), f32)
            moves[side * 4 + s].wait()
            for n in range(16):
                tile = b_ref[side * 4 + s, :, n * 128 : n * 128 + 128]
                total += tile * density_ref[n : n + 1, :]
            potential = jnp.sum(total, axis=1, keepdims=True)
            screened = screened_ref[pl.ds(pl.multiple_of(side * 256 + l * 64, 64), 64), :]
            source.append(2.0 * potential * points_refs[side * 4 + s][:, :V] - screened)
    source = halves(jnp.concatenate(source, axis=0))
    for ref, which in ((other_ref, 1 - core), (own_ref, core)):
        columns = halves(jnp.concatenate([columns_of(r, which) for r in points_refs], axis=0))
        done = product(source, columns, COLUMNS_BY_COLUMNS)
        for x in range(4):
            for h in range(2):
                for y in range(4):
                    v = ((x * 2 + h) * 4 + y) * 8
                    for l in range(4):
                        ref[x * 4 + y, h * 4 + l] = done[v : v + 8, l * 128 : l * 128 + 128]


def plane_sum_kernel(parts_ref, out_ref):
    for n in range(8):
        total = parts_ref[0, n]
        for i in range(1, 16):
            total += parts_ref[i, n]
        for i in range(8):
            out_ref[i, n] = total


def total_of(a):
    return jnp.sum(jnp.sum(a, axis=0, keepdims=True), axis=1, keepdims=True)


def sums_kernel(beta_ref, parts_ref, piece_ref, shifted_ref, sums_ref):
    beta_prev = beta_ref[0]
    sums = [jnp.zeros((8, 128), f32) for _ in range(4)]
    for n in range(8):
        total = parts_ref[0, n]
        for i in range(1, 8):
            total += parts_ref[i, n]
        q, p = piece_ref[n, 0], piece_ref[n, 1]
        shifted = piece_ref[n, 2] + total - middle_gap * q - beta_prev * p
        shifted_ref[n] = shifted
        sums = [sums[0] + shifted * shifted, sums[1] + shifted * q, sums[2] + q * q, sums[3] + q * p]
    line = jnp.zeros((1, 128), f32)
    for i in range(4):
        line = jnp.where(iota((1, 128), 1) == i, total_of(sums[i]), line)
    for i in range(32):
        sums_ref[i] = line


def last_kernel(beta_ref, at_ref, sums_ref, shifted_ref, q_ref, out_ref, coefficient_ref):
    line = sums_ref[0]
    for i in range(1, 32):
        line += sums_ref[i]
    line = line * inverse_size
    lane = iota((1, 128), 1)
    mean_ww, mean_wq, mean_qq, mean_qp = (
        jnp.sum(jnp.where(lane == i, line, 0.0), axis=1, keepdims=True) for i in range(4)
    )
    mean_qu = mean_wq + middle_gap * mean_qq + beta_ref[0] * mean_qp
    alpha = mean_qu / (mean_qq + epsilon)
    rest = alpha - middle_gap
    mean_rr = mean_ww - 2.0 * rest * mean_wq + rest * rest * mean_qq
    beta = jnp.sqrt(mean_rr + epsilon)
    shifted = shifted_ref[at_ref[3]]
    out_ref[...] = (shifted - rest * q_ref[...]) / beta
    coefficient_ref[...] = jnp.where(iota((1, 2), 1) == 0, alpha, beta)


def per_device(q, p, beta_prev, ev, ec, pv, pc, screened_coulomb, bare_coulomb):
    places = (K, X, Y, (H, L), L, H)
    at = jnp.stack([lax.axis_index(axis) for axis in places]).astype(jnp.int32)
    q, p = q[0], p[0]
    small = [pltpu.VMEM((8, 128), f32), pltpu.VMEM((8, 128), f32), pltpu.VMEM((1, 128), f32)]
    copies, points = local_kernel(
        first_kernel,
        [(8, 3, 8, 128), (64, V + C)],
        1 << 16,
        small + [pltpu.SemaphoreType.DMA((5,))],
    )(ev, far=(q, p, ec[None, :], pv, pc))
    piece = copies_to_all(copies, (H, L))
    own_half = from_all(piece[:, 0], (X, Y))
    other_half = from_partner(own_half)

    rows = [points] + [from_next(points, L, s) for s in (1, 2, 3)]
    rows += [from_partner(r) for r in rows]

    first, second = grid_swap(pv, 0), grid_swap(pv, 1)
    a, b = local_kernel(choose_kernel, [(64, V)] * 2, 1 << 16)(at, first, second)
    a_parts = jnp.stack([a] + [from_next(a, Y, s) for s in (1, 2, 3)])
    b_parts = jnp.stack([b] + [from_next(b, X, s) for s in (1, 2, 3)])
    a_parts = [a_parts] + [from_next(a_parts, X, s) for s in (1, 2, 3)]
    b_parts = [b_parts] + [from_next(b_parts, Y, s) for s in (1, 2, 3)]

    copies = local_kernel(amplitude_kernel, [(4, 72, V)], 1 << 27)(at, own_half, other_half, points)
    own_rows = copies_to_all(copies, L)
    other_rows = from_partner(own_rows)
    row_density = local_kernel(density_kernel, [(4, 128)], 1 << 10)(at, own_rows, other_rows)
    swapped = grid_swap(row_density, 0)
    far_density = from_all(swapped, Y).reshape(16, 128)

    screened = ()
    for turns in ((0, 1), (2, 3)):
        scratch = [pltpu.VMEM((8, 512, 128), f32), pltpu.VMEM((256, 512), f32)]
        scratch.append(pltpu.SemaphoreType.DMA((8,)))
        kernel = functools.partial(screened_kernel, turns)
        done = local_kernel(kernel, [(512, V)], 3 << 29, scratch, 16)(
            at, own_rows, other_rows, *a_parts, *b_parts, *screened, far=(screened_coulomb,)
        )
        screened = (done,)

    own_half, other_half = local_kernel(
        contribution_kernel,
        [(16, 8, 8, 128)] * 2,
        1 << 29,
        [pltpu.VMEM((8, 64, 2048), f32), pltpu.SemaphoreType.DMA((8,))],
        16,
    )(at, far_density, *screened, *rows, far=(bare_coulomb,))
    own_half += from_partner(other_half)
    parts = copies_to_all(own_half, (X, Y))
    copies = local_kernel(plane_sum_kernel, [(8, 8, 8, 128)], 1 << 18)(parts)
    parts = copies_to_all(copies, (H, L))

    shifted, sums = local_kernel(
        sums_kernel, [(8, 8, 128), (32, 1, 128)], 1 << 18
    )(beta_prev, parts, piece)
    sums = copies_to_all(sums, (X, Y, K))
    following, coefficients = local_kernel(
        last_kernel, [(8, 128), (1, 2)], 1 << 16, placed=False
    )(beta_prev, at, sums, shifted, arguments=(q,))
    return following[None], coefficients


def solution(mesh):
    torus = Mesh(mesh.devices.reshape(SIZES), AXES)
    return jax.shard_map(
        per_device,
        mesh=torus,
        in_specs=(
            P(None, ROW, COL),
            P(None, ROW, COL),
            P(),
            P(ROW),
            P(COL),
            P(AXES, None),
            P(AXES, None),
            P(ROW, COL),
            P(ROW, COL),
        ),
        out_specs=(P(None, ROW, COL), P()),
        check_vma=False,
    )
```

```python
import functools

import jax
import jax.numpy as jnp
from jax import lax
from jax.experimental import pallas as pl
from jax.experimental.pallas import tpu as pltpu
from jax.sharding import Mesh
from jax.sharding import PartitionSpec as P

V = 256
C = 1024
X, H, Y, L, K = "row_0", "row_1", "row_2", "col_0", "col_1"
SIZES = (4, 2, 4, 4, 2)
AXES = (X, H, Y, L, K)
ROW = (X, H, Y)
COL = (L, K)

f32 = jnp.float32
bf16 = jnp.bfloat16
epsilon = 1e-06
middle_gap = 2.5
inverse_size = 1.0 / (V * C)
SMEM = pl.BlockSpec(memory_space=pltpu.SMEM)
VMEM = pl.BlockSpec(memory_space=pltpu.VMEM)
HBM = pl.BlockSpec(memory_space=pltpu.HBM)


def copies_to_all(copies, axes):
    return lax.all_to_all(copies, axes, split_axis=0, concat_axis=0, tiled=True)


def from_all(block, axes):
    return copies_to_all(jnp.broadcast_to(block, (lax.axis_size(axes), *block.shape)), axes)


def from_partner(block):
    return lax.ppermute(block, K, [(0, 1), (1, 0)])


def from_next(block, axis, shift):
    return lax.ppermute(block, axis, [((i + shift) % 4, i) for i in range(4)])


def grid_swap(block, flip):
    pairs = []
    for a in range(4):
        for b in range(2):
            for c in range(4):
                for d in range(4):
                    for e in range(2):
                        source = (((a * 2 + b) * 4 + c) * 4 + d) * 2 + e
                        target = (((d * 2 + (e ^ flip)) * 4 + c) * 4 + a) * 2 + b
                        pairs.append((source, target))
    return lax.ppermute(block, AXES, pairs)


def iota(shape, dim):
    return lax.broadcasted_iota(jnp.int32, shape, dim)


def halves(a):
    high = a.astype(bf16)
    return high, (a - high.astype(f32)).astype(bf16)


def product(a, b, dims):
    def one(x, y):
        return lax.dot_general(x, y, (dims, ((), ())), preferred_element_type=f32)

    return one(a[0], b[0]) + (one(a[0], b[1]) + one(a[1], b[0]))


ROWS_BY_ROWS = ((1,), (1,))
PLAIN = ((1,), (0,))
COLUMNS_BY_COLUMNS = ((0,), (0,))


def local_kernel(body, out, flops, scratch=(), grant=8, placed=True):
    shapes = [pltpu.VMEM(s, f32) if placed else jax.ShapeDtypeStruct(s, f32) for s in out]
    many = len(shapes) > 1

    def call(*args, arguments=(), far=()):
        near = [
            a if a.ndim == 1 else pltpu.with_memory_space_constraint(a, pltpu.VMEM) for a in args
        ]
        near += list(arguments)
        far = [pltpu.with_memory_space_constraint(a, pltpu.HBM) for a in far]
        specs = [SMEM if a.ndim == 1 else VMEM for a in near] + [HBM] * len(far)
        return pl.pallas_call(
            body,
            out_shape=shapes if many else shapes[0],
            in_specs=specs,
            out_specs=[VMEM] * len(shapes) if many else VMEM,
            scratch_shapes=list(scratch),
            compiler_params=pltpu.CompilerParams(vmem_limit_bytes=grant << 20),
            cost_estimate=pl.CostEstimate(flops=flops, bytes_accessed=1 << 20, transcendentals=0),
        )(*near, *far)

    return call


def as_row(column, count):
    wide = jnp.broadcast_to(column, (count, V))
    same = iota((count, V), 0) == iota((count, V), 1)
    return jnp.sum(jnp.where(same, wide, 0.0), axis=0, keepdims=True)


def first_kernel(
    ev_ref, q_hbm, p_hbm, ec_hbm, pv_hbm, pc_hbm, out_ref, points_ref, q_ref, p_ref, ec_ref, sems
):
    pieces = (
        (q_hbm, q_ref),
        (p_hbm, p_ref),
        (ec_hbm, ec_ref),
        (pv_hbm, points_ref.at[:, :V]),
        (pc_hbm, points_ref.at[:, V:]),
    )
    moves = [pltpu.make_async_copy(a, b, sems.at[n]) for n, (a, b) in enumerate(pieces)]
    for move in moves:
        move.start()
    ev = jnp.zeros((8, 128), f32)
    for i in range(8):
        ev = jnp.where(iota((8, 128), 0) == i, ev_ref[i], ev)
    for move in moves[:3]:
        move.wait()
    gap_q = (ec_ref[...] - ev) * q_ref[...]
    for n in range(8):
        out_ref[n, 0] = q_ref[...]
        out_ref[n, 1] = p_ref[...]
        out_ref[n, 2] = gap_q
    for move in moves[3:]:
        move.wait()


def choose_kernel(at_ref, first_ref, second_ref, a_ref, b_ref):
    low = at_ref[5] == 0
    a_ref[...] = jnp.where(low, first_ref[...], second_ref[...])
    b_ref[...] = jnp.where(low, second_ref[...], first_ref[...])


def columns_of(points_ref, which):
    parts = [
        points_ref[:, pl.ds(pl.multiple_of(V + (2 * l + which) * 128, 128), 128)] for l in range(4)
    ]
    return jnp.concatenate(parts, axis=1)


def amplitude_kernel(at_ref, own_ref, other_ref, points_ref, out_ref):
    core = at_ref[0]
    total = jnp.zeros((64, V), f32)
    for ref, which in ((own_ref, core), (other_ref, 1 - core)):
        columns = [
            jnp.concatenate(
                [ref[x * 4 + y, h * 4 + l] for x in range(4) for h in range(2) for y in range(4)],
                axis=0,
            )
            for l in range(4)
        ]
        vectors = halves(jnp.concatenate(columns, axis=1))
        total += product(halves(columns_of(points_ref, which)), vectors, ROWS_BY_ROWS)
    density = as_row(jnp.sum(total * points_ref[:, :V], axis=1, keepdims=True), 64)
    tail = jnp.where(iota((8, V), 0) == 0, jnp.broadcast_to(density, (8, V)), 0.0)
    for n in range(4):
        out_ref[n, :64] = total
        out_ref[n, 64:] = tail


def density_kernel(at_ref, own_ref, other_ref, out_ref):
    south = at_ref[0] == 0
    for l in range(4):
        own, other = own_ref[l, 64:65, :128], other_ref[l, 64:65, :128]
        first, second = jnp.where(south, own, other), jnp.where(south, other, own)
        out_ref[l : l + 1, :] = first + pltpu.roll(second, 64, 1)


def screened_kernel(side, at_ref, rows_ref, *refs):
    a_refs, b_refs, (w_hbm, out_ref, w_ref, terms_ref, sems) = refs[:4], refs[4:8], refs[8:]
    which = at_ref[0] if side == 0 else 1 - at_ref[0]
    x, y = at_ref[1], at_ref[2]
    moves = []
    for l in range(4):
        rows = pl.ds(pl.multiple_of((2 * l + which) * 64, 64), 64)
        moves.append(pltpu.make_async_copy(w_hbm.at[rows, :], w_ref.at[l], sems.at[l]))
        moves[-1].start()
    pair = halves(jnp.concatenate([rows_ref[l, :64] for l in range(4)], axis=0))
    for t in range(4):
        points = [piece for s in range(4) for piece in (a_refs[t][s], b_refs[s][t])]
        points = halves(jnp.concatenate(points, axis=0))
        terms_ref[...] = product(pair, points, ROWS_BY_ROWS)
        for l in range(4):
            if t == 0:
                moves[l].wait()
            for s in range(4):
                at = pl.multiple_of(lax.rem(y + s, 4) * 512 + lax.rem(x + t, 4) * 128, 128)
                here = (slice(l * 64, l * 64 + 64), slice(s * 128, s * 128 + 128))
                terms_ref[here] = terms_ref[here] * w_ref[l, :, pl.ds(at, 128)]
        done = product(halves(terms_ref[...]), points, PLAIN)
        out_ref[...] = done if t == 0 else out_ref[...] + done


def contribution_kernel(at_ref, *refs):
    density_refs, screened_refs, points_refs = refs[:4], refs[4:6], refs[6:14]
    b_hbm, own_ref, other_ref, b_ref, density_ref, sems = refs[14:]
    core, y, z = at_ref[0], at_ref[2], at_ref[4]
    moves = []
    for side, which in enumerate((core, 1 - core)):
        for s in range(4):
            at = pl.multiple_of((2 * lax.rem(z + s, 4) + which) * 64, 64)
            n = side * 4 + s
            moves.append(
                pltpu.make_async_copy(b_hbm.at[pl.ds(at, 64), :], b_ref.at[n], sems.at[n])
            )
            moves[-1].start()
    for s in range(4):
        density_ref[lax.rem(y + s, 4)] = density_refs[s][...]
    columns = [
        halves(jnp.concatenate([columns_of(r, which) for r in points_refs], axis=0))
        for which in (1 - core, core)
    ]
    source = []
    for side in range(2):
        for s in range(4):
            l = lax.rem(z + s, 4)
            total = jnp.zeros((64, 128), f32)
            moves[side * 4 + s].wait()
            for n in range(16):
                tile = b_ref[side * 4 + s, :, n * 128 : n * 128 + 128]
                total += tile * density_ref[n // 4, n % 4 : n % 4 + 1, :]
            potential = jnp.sum(total, axis=1, keepdims=True)
            screened = screened_refs[side][pl.ds(pl.multiple_of(l * 64, 64), 64), :]
            source.append(2.0 * potential * points_refs[side * 4 + s][:, :V] - screened)
    source = halves(jnp.concatenate(source, axis=0))
    for ref, part in zip((other_ref, own_ref), columns):
        done = product(source, part, COLUMNS_BY_COLUMNS)
        for x in range(4):
            for h in range(2):
                for y in range(4):
                    v = ((x * 2 + h) * 4 + y) * 8
                    for l in range(4):
                        ref[x * 4 + y, h * 4 + l] = done[v : v + 8, l * 128 : l * 128 + 128]


def plane_sum_kernel(parts_ref, out_ref):
    for n in range(8):
        total = parts_ref[0, n]
        for i in range(1, 16):
            total += parts_ref[i, n]
        for i in range(8):
            out_ref[i, n] = total


def total_of(a):
    return jnp.sum(jnp.sum(a, axis=0, keepdims=True), axis=1, keepdims=True)


def sums_kernel(beta_ref, parts_ref, piece_ref, shifted_ref, sums_ref):
    beta_prev = beta_ref[0]
    sums = [jnp.zeros((8, 128), f32) for _ in range(4)]
    for n in range(8):
        total = parts_ref[0, n]
        for i in range(1, 8):
            total += parts_ref[i, n]
        q, p = piece_ref[n, 0], piece_ref[n, 1]
        shifted = piece_ref[n, 2] + total - middle_gap * q - beta_prev * p
        shifted_ref[n] = shifted
        sums = [sums[0] + shifted * shifted, sums[1] + shifted * q, sums[2] + q * q, sums[3] + q * p]
    line = jnp.zeros((1, 128), f32)
    for i in range(4):
        line = jnp.where(iota((1, 128), 1) == i, total_of(sums[i]), line)
    for i in range(32):
        sums_ref[i] = line


def last_kernel(beta_ref, at_ref, sums_ref, shifted_ref, q_ref, out_ref, coefficient_ref):
    line = sums_ref[0]
    for i in range(1, 32):
        line += sums_ref[i]
    line = line * inverse_size
    lane = iota((1, 128), 1)
    mean_ww, mean_wq, mean_qq, mean_qp = (
        jnp.sum(jnp.where(lane == i, line, 0.0), axis=1, keepdims=True) for i in range(4)
    )
    mean_qu = mean_wq + middle_gap * mean_qq + beta_ref[0] * mean_qp
    alpha = mean_qu / (mean_qq + epsilon)
    rest = alpha - middle_gap
    mean_rr = mean_ww - 2.0 * rest * mean_wq + rest * rest * mean_qq
    beta = jnp.sqrt(mean_rr + epsilon)
    shifted = shifted_ref[at_ref[3]]
    out_ref[...] = (shifted - rest * q_ref[...]) / beta
    coefficient_ref[...] = jnp.where(iota((1, 2), 1) == 0, alpha, beta)


def per_device(q, p, beta_prev, ev, ec, pv, pc, screened_coulomb, bare_coulomb):
    places = (K, X, Y, (H, L), L, H)
    at = jnp.stack([lax.axis_index(axis) for axis in places]).astype(jnp.int32)
    q, p = q[0], p[0]
    small = [pltpu.VMEM((8, 128), f32), pltpu.VMEM((8, 128), f32), pltpu.VMEM((1, 128), f32)]
    copies, points = local_kernel(
        first_kernel,
        [(8, 3, 8, 128), (64, V + C)],
        1 << 16,
        small + [pltpu.SemaphoreType.DMA((5,))],
    )(ev, far=(q, p, ec[None, :], pv, pc))
    piece = copies_to_all(copies, (H, L))
    own_half = from_all(piece[:, 0], (X, Y))
    other_half = from_partner(own_half)

    rows = [points] + [from_next(points, L, s) for s in (1, 2, 3)]
    rows += [from_partner(r) for r in rows]

    first, second = grid_swap(pv, 0), grid_swap(pv, 1)
    a, b = local_kernel(choose_kernel, [(64, V)] * 2, 1 << 16)(at, first, second)
    a_parts = jnp.stack([a] + [from_next(a, Y, s) for s in (1, 2, 3)])
    b_parts = jnp.stack([b] + [from_next(b, X, s) for s in (1, 2, 3)])
    a_parts = [a_parts] + [from_next(a_parts, X, s) for s in (1, 2, 3)]
    b_parts = [b_parts] + [from_next(b_parts, Y, s) for s in (1, 2, 3)]

    copies = local_kernel(amplitude_kernel, [(4, 72, V)], 1 << 27)(at, own_half, other_half, points)
    own_rows = copies_to_all(copies, L)
    other_rows = from_partner(own_rows)
    row_density = local_kernel(density_kernel, [(4, 128)], 1 << 10)(at, own_rows, other_rows)
    swapped = grid_swap(row_density, 0)
    far_density = [swapped] + [from_next(swapped, Y, s) for s in (1, 2, 3)]

    screened = []
    for side, there in enumerate((own_rows, other_rows)):
        scratch = [pltpu.VMEM((4, 64, 2048), f32), pltpu.VMEM((256, 512), f32)]
        scratch.append(pltpu.SemaphoreType.DMA((4,)))
        kernel = functools.partial(screened_kernel, side)
        screened.append(
            local_kernel(kernel, [(256, V)], 3 << 29, scratch, 16)(
                at, there, *a_parts, *b_parts, far=(screened_coulomb,)
            )
        )

    scratch = [pltpu.VMEM((8, 64, 2048), f32), pltpu.VMEM((4, 4, 128), f32)]
    scratch.append(pltpu.SemaphoreType.DMA((8,)))
    own_half, other_half = local_kernel(
        contribution_kernel, [(16, 8, 8, 128)] * 2, 1 << 29, scratch, 16
    )(at, *far_density, *screened, *rows, far=(bare_coulomb,))
    own_half += from_partner(other_half)
    parts = copies_to_all(own_half, (X, Y))
    copies = local_kernel(plane_sum_kernel, [(8, 8, 8, 128)], 1 << 18)(parts)
    parts = copies_to_all(copies, (H, L))

    shifted, sums = local_kernel(
        sums_kernel, [(8, 8, 128), (32, 1, 128)], 1 << 18
    )(beta_prev, parts, piece)
    sums = copies_to_all(sums, (X, Y, K))
    following, coefficients = local_kernel(
        last_kernel, [(8, 128), (1, 2)], 1 << 16, placed=False
    )(beta_prev, at, sums, shifted, arguments=(q,))
    return following[None], coefficients


def solution(mesh):
    torus = Mesh(mesh.devices.reshape(SIZES), AXES)
    return jax.shard_map(
        per_device,
        mesh=torus,
        in_specs=(
            P(None, ROW, COL),
            P(None, ROW, COL),
            P(),
            P(ROW),
            P(COL),
            P(AXES, None),
            P(AXES, None),
            P(ROW, COL),
            P(ROW, COL),
        ),
        out_specs=(P(None, ROW, COL), P()),
        check_vma=False,
    )
```
